32 devices in a mesh: vocab: 8 (over z, x), group: 4 (over y, core).
Axes of the slice: x: 2, y: 2, z: 4, core: 2. Of those that a mesh axis runs over, the one named last changes fastest.
Arguments:
- hidden_states: bfloat16 [512, 4096], P(('group', 'vocab')), parts along dimension 0, may hold values from -32 to 32
- head_weight: bfloat16 [4096, 19456], P(None, 'vocab'), may hold values from -1 to 1
- pick_index: int32 [512, 64], P('group'), parts along dimension 0, may hold values from 0 to 19455, as said below
- owner_order: int32 [512], P('group'), parts along dimension 0, may hold values from 0 to 127, each once
Outputs:
- token_logprobs: float32 [512, 64], P(('group', 'vocab')), parts along dimension 0
- token_logtotal: float32 [512], P(('group', 'vocab')), parts along dimension 0
The draws below stay inside these ranges and needn't reach their ends.
There are 4 independent parts, one for each index of `group`. The reference program is written for one: setup_inputs(seed, part) draws one part's arguments, and reference() takes and returns one part's arrays. A program takes and returns all parts, laid end to end along the dimension named above; an argument that names none is the same for every part. Nothing has to cross between parts.
Inputs may be any that keep to these rules, and one draw needn't show every extreme that they name: `pick_index`: each row holds 64 distinct vocabulary entries. `owner_order`: each token appears once.
All inputs are finite; a program needn't handle non-finite values.
Results may differ from the reference program's by a relative error of at most 0.0003.
Values may be sent and summed in bfloat16 or wider, within the bound.
A program may use at most 128 MiB of HBM per device.

```python
import math
import jax
import jax.numpy as jnp

D = 4096
K = 64
TOKENS = 128
VOCAB = 19456


def weight_column(key, column):
    column_key = jax.random.fold_in(jax.random.fold_in(key, 7), column)
    values = jnp.clip(jax.random.normal(column_key, (D,), jnp.float32), -6.0, 6.0)
    factor = jnp.exp(jax.random.uniform(jax.random.fold_in(column_key, 1), (), jnp.float32, math.log(0.7), math.log(1.4)))
    position = column.astype(jnp.float32) / VOCAB
    scale = 3.0 * jnp.exp(0.13 * position) * factor
    return values * scale / math.sqrt(D)


def draw_head_weight(key, part):
    columns = jax.vmap(lambda column: weight_column(key, column))(jnp.arange(VOCAB, dtype=jnp.int32))
    result = columns.T
    return jnp.clip(result, -1.0, 1.0).astype(jnp.bfloat16)


def draw_hidden_states(key, part):
    base_key = jax.random.fold_in(key, 11)
    result = jnp.clip(jax.random.normal(base_key, (TOKENS, D), jnp.float32), -6.0, 6.0)
    return jnp.clip(result, -32.0, 32.0).astype(jnp.bfloat16)


def draw_pick_index(key, part):
    base_key = jax.random.fold_in(key, 21)
    raw_draw = jax.random.randint(base_key, (TOKENS, K), 0, VOCAB - K + 1)
    spread = jnp.sort(raw_draw, axis=1) + jnp.arange(K, dtype=jnp.int32)[None, :]
    scores = jax.random.randint(jax.random.fold_in(base_key, 1), (TOKENS, K), 0, 1 << 20) * K + jnp.arange(K, dtype=jnp.int32)[None, :]
    shuffle = jnp.argsort(scores, axis=1, stable=True)
    return jnp.take_along_axis(spread, shuffle, axis=1).astype(jnp.int32)


def setup_inputs(seed: int = 0, part: int = 0) -> dict:
    streams_of = jax.random.split(jax.random.key(seed), 5)
    own_keys = jax.random.split(jax.random.fold_in(streams_of[4], part), 5)
    hidden_states = draw_hidden_states(jax.random.fold_in(jax.random.fold_in(streams_of[4], part), 71), part)
    head_weight = draw_head_weight(jax.random.fold_in(streams_of[4], 71), part)
    pick_index = draw_pick_index(jax.random.fold_in(jax.random.fold_in(streams_of[4], part), 71), part)
    owner_order = jax.random.permutation(own_keys[3], TOKENS).astype(jnp.int32)
    return {"hidden_states": hidden_states, "head_weight": head_weight, "pick_index": pick_index, "owner_order": owner_order}


def reference(hidden_states, head_weight, pick_index, owner_order):
    logits = jnp.dot(hidden_states, head_weight, preferred_element_type=jnp.float32)
    row_max = jnp.max(logits, axis=1)
    log_total = row_max + jnp.log(jnp.sum(jnp.exp(logits - row_max[:, None]), axis=1))
    picked = jnp.take_along_axis(logits, pick_index, axis=1) - log_total[:, None]
    return picked[owner_order], log_total[owner_order]
```

```python
import functools

import jax
import jax.numpy as jnp
from jax import lax
from jax.experimental import pallas as pl
from jax.experimental.pallas import tpu as pltpu
from jax.sharding import PartitionSpec as P

MESH = pl.DeviceIdType.MESH
LANES = 128


def kernel(
    n, chunks,
    hid, weight, pick, order,
    logprobs, logtotal,
    gathered, held, logits, stage, outbox, inbox,
    weight_sem, own_sem, far_send, far_recv, near_send, near_recv, end_send, end_recv,
):
    me = lax.axis_index("vocab")
    rows, depth = hid.shape
    tokens = gathered.shape[0]
    width = weight.shape[1]
    picks = pick.shape[1]
    kc = depth // chunks
    pair = 2 if n % 2 == 0 else 1
    outer = n // pair
    pos, side = me // pair, me % pair
    partner = me + 1 - 2 * side

    def columns(c):
        return pl.ds(c * kc, kc)

    def block(owner, c):
        return gathered.at[pl.ds(pl.multiple_of(owner * rows, rows), rows), columns(c)]

    weight_copies = []
    for c in range(chunks):
        copy = pltpu.make_async_copy(weight.at[columns(c), :], held.at[columns(c), :], weight_sem.at[c])
        copy.start()
        weight_copies.append(copy)
    own = pltpu.make_async_copy(hid, gathered.at[pl.ds(pl.multiple_of(me * rows, rows), rows), :], own_sem)
    own.start()

    barrier = pltpu.get_barrier_semaphore()
    for j in range(1, n):
        pl.semaphore_signal(barrier, inc=1, device_id={"vocab": lax.rem(me + j, n)}, device_id_type=MESH)
    pl.semaphore_wait(barrier, n - 1)

    far = [[] for _ in range(chunks)]
    near = [[] for _ in range(chunks)]
    for c in range(chunks):
        for j in range(1, outer):
            copy = pltpu.make_async_remote_copy(
                src_ref=hid.at[:, columns(c)], dst_ref=block(me, c),
                send_sem=far_send.at[c, j - 1], recv_sem=far_recv.at[c, j - 1],
                device_id={"vocab": lax.rem(pos + j, outer) * pair + side}, device_id_type=MESH,
            )
            copy.start()
            far[c].append(copy)
        if pair == 2:
            copy = pltpu.make_async_remote_copy(
                src_ref=hid.at[:, columns(c)], dst_ref=block(me, c),
                send_sem=near_send.at[c, 0], recv_sem=near_recv.at[c, 0],
                device_id={"vocab": partner}, device_id_type=MESH,
            )
            copy.start()
            near[c].append(copy)

    for step in range(chunks + 1):
        if step < chunks:
            c = step
            for j in range(1, outer):
                far[c][j - 1].wait_recv()
                if pair == 2:
                    source = lax.rem(pos - j + outer, outer) * pair + side
                    copy = pltpu.make_async_remote_copy(
                        src_ref=block(source, c), dst_ref=block(source, c),
                        send_sem=near_send.at[c, j], recv_sem=near_recv.at[c, j],
                        device_id={"vocab": partner}, device_id_type=MESH,
                    )
                    copy.start()
                    near[c].append(copy)
        if step >= 1:
            c = step - 1
            if c == 0:
                own.wait()
            for copy in near[c]:
                copy.wait_recv()
            weight_copies[c].wait()
            left = gathered[:, columns(c)]
            for start in range(0, width, 256):
                span = pl.ds(start, min(256, width - start))
                part = jnp.dot(left, held[columns(c), span], preferred_element_type=jnp.float32)
                if c == 0:
                    logits[:, span] = part
                else:
                    logits[:, span] += part

    group = 32

    def rows_of(i, carry):
        at = pl.ds(pl.multiple_of(i * group, group), group)
        own_pick = pick[at, :] - me * width
        own_pick = jnp.concatenate([own_pick] * (LANES // picks), axis=1)
        tile, lane = own_pick >> 7, own_pick & (LANES - 1)
        tiles = [logits[at, pl.ds(v * LANES, LANES)] for v in range(width // LANES)]
        top = functools.reduce(jnp.maximum, tiles)
        top = jnp.max(top, axis=1, keepdims=True)
        total = functools.reduce(jnp.add, [jnp.exp(x - top) for x in tiles])
        total = jnp.sum(total, axis=1, keepdims=True)
        found = jnp.zeros((group, LANES), jnp.float32)
        for v, x in enumerate(tiles):
            found = jnp.where(tile == v, jnp.take_along_axis(x, lane, axis=1, mode="promise_in_bounds"), found)
        at_lane = lax.broadcasted_iota(jnp.int32, (group, LANES), 1)
        found = jnp.where(at_lane == picks, top, found)
        found = jnp.where(at_lane == picks + 1, total, found)
        stage[at, :] = found
        return carry

    lax.fori_loop(0, tokens // group, rows_of, 0)

    def permute(i, carry):
        for k in range(8):
            r = i * 8 + k
            outbox[pl.ds(r, 1), :] = stage[pl.ds(order[r], 1), :]
        return carry

    lax.fori_loop(0, tokens // 8, permute, 0)

    end = []
    for j in range(1, n):
        to = lax.rem(me + j, n)
        copy = pltpu.make_async_remote_copy(
            src_ref=outbox.at[pl.ds(pl.multiple_of(to * rows, rows), rows), :], dst_ref=inbox.at[j - 1],
            send_sem=end_send.at[j - 1], recv_sem=end_recv.at[j - 1],
            device_id={"vocab": to}, device_id_type=MESH,
        )
        copy.start()
        end.append(copy)
    for c in range(chunks):
        for copy in far[c] + near[c]:
            copy.wait_send()
    for copy in end:
        copy.wait_recv()
    parts = [outbox[pl.ds(pl.multiple_of(me * rows, rows), rows), :]] + [inbox[j] for j in range(n - 1)]
    tops = [x[:, picks:picks + 1] for x in parts]
    top = functools.reduce(jnp.maximum, tops)
    total = functools.reduce(jnp.add, [x[:, picks + 1:picks + 2] * jnp.exp(t - top) for x, t in zip(parts, tops)])
    log_total = top + jnp.log(total)
    logprobs[...] = functools.reduce(jnp.add, [x[:, :picks] for x in parts]) - log_total
    diagonal = lax.broadcasted_iota(jnp.int32, (rows, rows), 0) == lax.broadcasted_iota(jnp.int32, (rows, rows), 1)
    logtotal[...] = jnp.sum(jnp.where(diagonal, log_total, 0.0), axis=0, keepdims=True)
    for copy in end:
        copy.wait_send()


def local(hidden_states, head_weight, pick_index, owner_order):
    n = lax.axis_size("vocab")
    rows, depth = hidden_states.shape
    width = head_weight.shape[1]
    tokens, picks = pick_index.shape
    chunks = 8
    pair = 2 if n % 2 == 0 else 1
    outer = n // pair
    dma = pltpu.SemaphoreType.DMA
    logprobs, logtotal = pl.pallas_call(
        functools.partial(kernel, n, chunks),
        out_shape=(
            jax.ShapeDtypeStruct((rows, picks), jnp.float32),
            jax.ShapeDtypeStruct((1, rows), jnp.float32),
        ),
        in_specs=[
            pl.BlockSpec(memory_space=pl.ANY),
            pl.BlockSpec(memory_space=pl.ANY),
            pl.BlockSpec(memory_space=pltpu.VMEM),
            pl.BlockSpec(memory_space=pltpu.SMEM),
        ],
        out_specs=(pl.BlockSpec(memory_space=pltpu.VMEM), pl.BlockSpec(memory_space=pltpu.VMEM)),
        scratch_shapes=[
            pltpu.VMEM((tokens, depth), jnp.bfloat16),
            pltpu.VMEM((depth, width), jnp.bfloat16),
            pltpu.VMEM((tokens, width), jnp.float32),
            pltpu.VMEM((tokens, LANES), jnp.float32),
            pltpu.VMEM((tokens, LANES), jnp.float32),
            pltpu.VMEM((n - 1, rows, LANES), jnp.float32),
            dma((chunks,)),
            dma(()),
            dma((chunks, max(outer - 1, 1))),
            dma((chunks, max(outer - 1, 1))),
            dma((chunks, outer)),
            dma((chunks, outer)),
            dma((n - 1,)),
            dma((n - 1,)),
        ],
        compiler_params=pltpu.CompilerParams(
            collective_id=0, has_side_effects=True, vmem_limit_bytes=60 * 1024 * 1024
        ),
    )(hidden_states, head_weight, pick_index, owner_order)
    return logprobs, logtotal.reshape(rows)


def solution(mesh):
    in_specs = (P(("group", "vocab"), None), P(None, "vocab"), P("group", None), P("group"))
    out_specs = (P(("group", "vocab"), None), P(("group", "vocab")))
    return jax.shard_map(local, mesh=mesh, in_specs=in_specs, out_specs=out_specs, check_vma=False)
```

```python
import functools

import jax
import jax.numpy as jnp
from jax import lax
from jax.experimental import pallas as pl
from jax.experimental.pallas import tpu as pltpu
from jax.sharding import PartitionSpec as P

MESH = pl.DeviceIdType.MESH
LANES = 128


def kernel(
    n, chunks,
    hid, weight, pick, order,
    logprobs, logtotal,
    gathered, held, logits, wanted, stage, outbox, inbox,
    weight_sem, own_sem, up_send, up_recv, down_send, down_recv, near_send, near_recv, end_send, end_recv,
):
    me = lax.axis_index("vocab")
    rows, depth = hid.shape
    tokens = gathered.shape[0]
    width = weight.shape[1]
    picks = pick.shape[0]
    kc = depth // chunks
    pair = 2 if n % 2 == 0 else 1
    outer = n // pair
    pos, side = me // pair, me % pair
    partner = me + 1 - 2 * side

    def columns(c):
        return pl.ds(c * kc, kc)

    def block(owner, c):
        return gathered.at[pl.ds(pl.multiple_of(owner * rows, rows), rows), columns(c)]

    weight_copies = []
    for c in range(chunks):
        copy = pltpu.make_async_copy(weight.at[columns(c), :], held.at[columns(c), :], weight_sem.at[c])
        copy.start()
        weight_copies.append(copy)
    own = pltpu.make_async_copy(hid, gathered.at[pl.ds(pl.multiple_of(me * rows, rows), rows), :], own_sem)
    own.start()

    barrier = pltpu.get_barrier_semaphore()
    for j in range(1, n):
        pl.semaphore_signal(barrier, inc=1, device_id={"vocab": lax.rem(me + j, n)}, device_id_type=MESH)
    wanted[...] = jnp.concatenate([pick[...]] * (LANES // picks), axis=0).T - me * width
    pl.semaphore_wait(barrier, n - 1)

    def far(sems, c, d, step, hop):
        owner = (pos - step * d) * pair + side
        there = block(owner, c)
        send, recv = sems
        return pltpu.make_async_remote_copy(
            src_ref=hid.at[:, columns(c)] if d == 0 else there, dst_ref=there,
            send_sem=send.at[c, d], recv_sem=recv.at[c, d + hop],
            device_id={"vocab": lax.rem(me + step * pair + n, n)}, device_id_type=MESH,
        )

    def near(c, owner, slot):
        there = block(owner, c)
        return pltpu.make_async_remote_copy(
            src_ref=hid.at[:, columns(c)] if slot == 0 else there, dst_ref=there,
            send_sem=near_send.at[c, slot], recv_sem=near_recv.at[c, slot],
            device_id={"vocab": partner}, device_id_type=MESH,
        )

    lines = (
        ((up_send, up_recv), 1, 0, lambda d: pos >= d, pos < outer - 1),
        ((down_send, down_recv), -1, outer - 1, lambda d: pos + d < outer, pos > 0),
    )
    for c in range(chunks):
        for sems, step, base, has, onward in lines:
            if outer > 1:
                @pl.when(onward)
                def _():
                    far(sems, c, 0, step, 0).start()
        if pair == 2:
            near(c, me, 0).start()

    def relay(c, d):
        for sems, step, base, has, onward in lines:
            @pl.when(has(d))
            def _():
                far(sems, c, d, step, -1).wait_recv()
                if d < outer - 1:
                    @pl.when(onward)
                    def _():
                        far(sems, c, d, step, 0).start()
                if pair == 2:
                    near(c, (pos - step * d) * pair + side, base + d).start()

    def multiply(c):
        if c == 0:
            own.wait()
        if pair == 2:
            near(c, me + 1 - 2 * side, 0).wait_recv()
            for d in range(1, outer):
                for sems, step, base, has, onward in lines:
                    @pl.when(has(d))
                    def _():
                        near(c, (pos - step * d) * pair + 1 - side, base + d).wait_recv()
        weight_copies[c].wait()
        left = gathered[:, columns(c)]
        for start in range(0, width, 256):
            span = pl.ds(start, min(256, width - start))
            part = jnp.dot(left, held[columns(c), span], preferred_element_type=jnp.float32)
            if c == 0:
                logits[:, span] = part
            else:
                logits[:, span] += part

    for d in range(1, outer - 1):
        for c in range(chunks):
            relay(c, d)
    for c in range(chunks):
        if outer > 1:
            relay(c, outer - 1)
        if c >= 1:
            multiply(c - 1)
    multiply(chunks - 1)

    group = 32

    def rows_of(i, carry):
        at = pl.ds(pl.multiple_of(i * group, group), group)
        own_pick = wanted[at, :]
        tile, lane = own_pick >> 7, own_pick & (LANES - 1)
        tiles = [logits[at, pl.ds(v * LANES, LANES)] for v in range(width // LANES)]
        top = functools.reduce(jnp.maximum, tiles)
        top = jnp.max(top, axis=1, keepdims=True)
        total = functools.reduce(jnp.add, [jnp.exp(x - top) for x in tiles])
        total = jnp.sum(total, axis=1, keepdims=True)
        found = jnp.zeros((group, LANES), jnp.float32)
        for v, x in enumerate(tiles):
            found = jnp.where(tile == v, jnp.take_along_axis(x, lane, axis=1, mode="promise_in_bounds"), found)
        at_lane = lax.broadcasted_iota(jnp.int32, (group, LANES), 1)
        found = jnp.where(at_lane == picks, top, found)
        found = jnp.where(at_lane == picks + 1, total, found)
        stage[at, :] = found
        return carry

    lax.fori_loop(0, tokens // group, rows_of, 0)

    def permute(i, carry):
        for k in range(8):
            r = i * 8 + k
            outbox[pl.ds(r, 1), :] = stage[pl.ds(order[r], 1), :]
        return carry

    lax.fori_loop(0, tokens // 8, permute, 0)

    end = []
    for j in range(1, n):
        to = lax.rem(me + j, n)
        copy = pltpu.make_async_remote_copy(
            src_ref=outbox.at[pl.ds(pl.multiple_of(to * rows, rows), rows), :], dst_ref=inbox.at[j - 1],
            send_sem=end_send.at[j - 1], recv_sem=end_recv.at[j - 1],
            device_id={"vocab": to}, device_id_type=MESH,
        )
        copy.start()
        end.append(copy)
    for c in range(chunks):
        if pair == 2:
            near(c, me, 0).wait_send()
        for sems, step, base, has, onward in lines:
            for d in range(outer - 1):
                @pl.when(jnp.logical_and(has(d), onward))
                def _():
                    far(sems, c, d, step, 0).wait_send()
            if pair == 2:
                for d in range(1, outer):
                    @pl.when(has(d))
                    def _():
                        near(c, (pos - step * d) * pair + side, base + d).wait_send()
    for copy in end:
        copy.wait_recv()
    parts = [outbox[pl.ds(pl.multiple_of(me * rows, rows), rows), :]] + [inbox[j] for j in range(n - 1)]
    tops = [x[:, picks:picks + 1] for x in parts]
    top = functools.reduce(jnp.maximum, tops)
    total = functools.reduce(jnp.add, [x[:, picks + 1:picks + 2] * jnp.exp(t - top) for x, t in zip(parts, tops)])
    log_total = top + jnp.log(total)
    logprobs[...] = functools.reduce(jnp.add, [x[:, :picks] for x in parts]) - log_total
    diagonal = lax.broadcasted_iota(jnp.int32, (rows, rows), 0) == lax.broadcasted_iota(jnp.int32, (rows, rows), 1)
    logtotal[...] = jnp.sum(jnp.where(diagonal, log_total, 0.0), axis=0, keepdims=True)
    for copy in end:
        copy.wait_send()


def finish(logprobs, logtotal, logprobs_out, logtotal_out):
    logprobs_out[...] = logprobs[...]
    logtotal_out[...] = logtotal[...]


def local(hidden_states, head_weight, pick_index, owner_order):
    n = lax.axis_size("vocab")
    rows, depth = hidden_states.shape
    width = head_weight.shape[1]
    tokens, picks = pick_index.shape
    chunks = 2
    pair = 2 if n % 2 == 0 else 1
    outer = n // pair
    dma = pltpu.SemaphoreType.DMA
    logprobs, logtotal = pl.pallas_call(
        functools.partial(kernel, n, chunks),
        out_shape=(
            jax.ShapeDtypeStruct((rows, picks), jnp.float32),
            jax.ShapeDtypeStruct((1, rows), jnp.float32),
        ),
        in_specs=[
            pl.BlockSpec(memory_space=pl.ANY),
            pl.BlockSpec(memory_space=pl.ANY),
            pl.BlockSpec(memory_space=pltpu.VMEM),
            pl.BlockSpec(memory_space=pltpu.SMEM),
        ],
        out_specs=(pl.BlockSpec(memory_space=pltpu.VMEM), pl.BlockSpec(memory_space=pltpu.VMEM)),
        scratch_shapes=[
            pltpu.VMEM((tokens, depth), jnp.bfloat16),
            pltpu.VMEM((depth, width), jnp.bfloat16),
            pltpu.VMEM((tokens, width), jnp.float32),
            pltpu.VMEM((tokens, LANES), jnp.int32),
            pltpu.VMEM((tokens, LANES), jnp.float32),
            pltpu.VMEM((tokens, LANES), jnp.float32),
            pltpu.VMEM((n - 1, rows, LANES), jnp.float32),
            dma((chunks,)),
            dma(()),
            dma((chunks, outer)),
            dma((chunks, outer)),
            dma((chunks, outer)),
            dma((chunks, outer)),
            dma((chunks, 2 * outer - 1)),
            dma((chunks, 2 * outer - 1)),
            dma((n - 1,)),
            dma((n - 1,)),
        ],
        compiler_params=pltpu.CompilerParams(
            collective_id=0, has_side_effects=True, vmem_limit_bytes=60 * 1024 * 1024
        ),
    )(hidden_states, head_weight, pick_index.T, owner_order)
    logprobs, logtotal = pl.pallas_call(
        finish,
        out_shape=(
            jax.ShapeDtypeStruct((rows, picks), jnp.float32),
            jax.ShapeDtypeStruct((1, rows), jnp.float32),
        ),
    )(logprobs, logtotal)
    return logprobs, logtotal.reshape(rows)


def solution(mesh):
    in_specs = (P(("group", "vocab"), None), P(None, "vocab"), P("group", None), P("group"))
    out_specs = (P(("group", "vocab"), None), P(("group", "vocab")))
    return jax.shard_map(local, mesh=mesh, in_specs=in_specs, out_specs=out_specs, check_vma=False)
```
